32 devices in a mesh: members: 2 (over y), comp: 4 (over z), lat: 2 (over x), sub: 2 (over core).
Axes of the slice: x: 2, y: 2, z: 4, core: 2. Of those that a mesh axis runs over, the one named last changes fastest.
Arguments:
- spectrum: float32 [1920, 4096], P('comp', ('members', 'lat', 'sub')), parts along dimension 1, may hold values from 0.05 to 2
- sea_mask: int32 [4096], P(('members', 'lat', 'sub')), parts along dimension 0, may hold values 0 or 1
- neighbours: int32 [4, 4096], P(None, ('members', 'lat', 'sub')), parts along dimension 1, may hold values from 0 to 2047, as said below
- substeps: int32 [30], replicated, may hold values from 1 to 6, as said below
- courant: float32 [30], replicated, may hold values from 0.2 to 0.7
- source_operator: bfloat16 [1920, 1920], P('sub'), may hold values from -0.125 to 0.125
Outputs:
- new_spectrum: float32 [1920, 4096], P('comp', ('members', 'lat', 'sub')), parts along dimension 1
The draws below stay inside these ranges and needn't reach their ends.
There are 2 independent parts, one for each index of `members`. The reference program is written for one: setup_inputs(seed, part) draws one part's arguments, and reference() takes and returns one part's arrays. A program takes and returns all parts, laid end to end along the dimension named above; an argument that names none is the same for every part. Nothing has to cross between parts.
Inputs may be any that keep to these rules, and one draw needn't show every extreme that they name: Non-increasing with the band; the first band takes 6 substeps and the last band one. Points are numbered row by row, 256 to a row. The west and east neighbours lie in the same row, one or two columns away, wrapping around the row. The south neighbour lies in the row before and the north neighbour in the row after, within one column (wrapping); on the first and last row of the member's grid that neighbour is the point itself.
All inputs are finite; a program needn't handle non-finite values. No bound on the sum of `sea_mask` on one device may be relied on, other than what follows from the above.
Results may differ from the reference program's by a relative error of at most 0.0015.
Values may be sent and summed in bfloat16 or wider, within the bound.
A program may use at most 64 MiB of HBM per device.

```python
import math
import jax
import jax.numpy as jnp

NF = 30
ND = 64
NBINS = 1920
NLON = 256
MAXSTEPS = 6
SRC_STEPS = 4
P_SIZE = 2048


def draw_neighbours(key, part):
    rows_all = P_SIZE // NLON
    position = jnp.arange(P_SIZE, dtype=jnp.int32)
    row_number = position // NLON
    column = position % NLON
    key_list = jax.random.split(key, 4)
    west_step = jax.random.randint(key_list[0], (P_SIZE,), 1, 3).astype(jnp.int32)
    east_step = jax.random.randint(key_list[1], (P_SIZE,), 1, 3).astype(jnp.int32)
    south_step = jax.random.randint(key_list[2], (P_SIZE,), -1, 2).astype(jnp.int32)
    north_step = jax.random.randint(key_list[3], (P_SIZE,), -1, 2).astype(jnp.int32)
    west_index = row_number * NLON + (column - west_step) % NLON
    east_index = row_number * NLON + (column + east_step) % NLON
    south_index = jnp.where(row_number > 0, (row_number - 1) * NLON + (column + south_step) % NLON, position)
    north_index = jnp.where(row_number < rows_all - 1, (row_number + 1) * NLON + (column + north_step) % NLON, position)
    return jnp.stack([west_index, east_index, south_index, north_index]).astype(jnp.int32)


def draw_substeps(key, part):
    raw_counts = jax.random.randint(key, (NF,), 1, MAXSTEPS + 1).astype(jnp.int32)
    raw_counts = raw_counts.at[0].set(MAXSTEPS).at[NF - 1].set(1)
    return (-jnp.sort(-raw_counts)).astype(jnp.int32)


def set_ends(entries, stream_key, low, largest):
    extent = entries.shape
    place = [jax.random.randint(jax.random.fold_in(stream_key, axis), (), 0, extent[axis]) for axis in range(len(extent))]
    entries = entries.at[tuple(place)].set(low)
    longest = extent.index(max(extent))
    place[longest] = (place[longest] + 1) % extent[longest]
    return entries.at[tuple(place)].set(largest)


def shard_levels(own_key, extent, shards, low, largest):
    gain, own = 1.0, jax.random.fold_in(own_key, 6)
    for dim, shards_of in shards:
        heights = jnp.exp(jax.random.uniform(jax.random.fold_in(own, dim), (shards_of,), jnp.float32, low / len(shards), largest / len(shards)))
        gain = gain * jnp.repeat(heights, extent[dim] // shards_of).reshape([-1 if axis == dim else 1 for axis in range(len(extent))])
    return gain


def normal_values(own_key, extent, spread, reach, pieces=(), kind=jnp.bfloat16):
    drawn = jax.random.normal(own_key, extent, jnp.float32) * spread
    if len(pieces) > 0:
        drawn = shard_levels(own_key, extent, pieces, -0.22, 0.18) * drawn
    return jnp.clip(drawn, min=-reach, max=reach).astype(kind)


def setup_inputs(seed: int = 0, part: int = 0) -> dict:
    arg_keys = jax.random.split(jax.random.key(seed), 7)
    own_keys = jax.random.split(jax.random.fold_in(arg_keys[6], part), 7)
    return {
        "spectrum": jnp.clip(jnp.exp(math.log(2.0) - 3.6888794 * jax.random.uniform(own_keys[0], (NBINS, P_SIZE), jnp.float32) ** shard_levels(own_keys[0], (NBINS, P_SIZE), ((0, 4), (1, 4)), -0.2, 0.2)), 0.05, 2.0),
        "sea_mask": set_ends((jax.random.randint(own_keys[1], (P_SIZE,), 0, 5) < 4).astype(jnp.int32), jax.random.fold_in(own_keys[1], 1), 0, 1),
        "neighbours": draw_neighbours(jax.random.fold_in(jax.random.fold_in(arg_keys[6], part), 71), part),
        "substeps": draw_substeps(jax.random.fold_in(arg_keys[6], 71), part),
        "courant": jnp.clip(jax.random.uniform(arg_keys[4], (NF,), jnp.float32, 0.2, 0.7), 0.2, 0.7),
        "source_operator": normal_values(arg_keys[5], (NBINS, NBINS), NBINS ** -0.5, 0.125, ((0, 2),)),
    }


STEP_SIZE = 0.1


def reference(spectrum, sea_mask, neighbours, substeps, courant, source_operator):
    bin_index = jnp.arange(NF * ND, dtype=jnp.int32)
    frequency = bin_index // ND
    direction = bin_index % ND
    angles = (direction.astype(jnp.float32) + 0.5) * (2.0 * math.pi / ND)
    cosine = jnp.cos(angles)
    sine_dir = jnp.sin(angles)
    bin_speed = courant[frequency]
    weight_x = bin_speed * jnp.abs(cosine)
    weight_y = bin_speed * jnp.abs(sine_dir)
    bin_steps = substeps[frequency]
    sea_float = sea_mask.astype(jnp.float32)
    field_now = sea_float[None, :] * spectrum
    for substep in range(MAXSTEPS):
        west_vals = field_now[:, neighbours[0]]
        east_vals = field_now[:, neighbours[1]]
        south_vals = field_now[:, neighbours[2]]
        north_vals = field_now[:, neighbours[3]]
        upwind_lon = jnp.where((cosine > 0)[:, None], west_vals, east_vals)
        upwind_lat = jnp.where((sine_dir > 0)[:, None], south_vals, north_vals)
        advanced = sea_float[None, :] * (field_now - weight_x[:, None] * (field_now - upwind_lon)
                                         - weight_y[:, None] * (field_now - upwind_lat))
        field_now = jnp.where((substep < bin_steps)[:, None], advanced, field_now)
    propagated = field_now
    start_spec = propagated.astype(jnp.bfloat16)
    state_now = start_spec.astype(jnp.float32)
    for source_step in range(SRC_STEPS):
        driving = jnp.dot(source_operator, state_now.astype(jnp.bfloat16), preferred_element_type=jnp.float32)
        state_now = state_now + STEP_SIZE * state_now * driving
    increment = (state_now - start_spec.astype(jnp.float32)).astype(jnp.bfloat16)
    return sea_float[None, :] * (propagated + increment.astype(jnp.float32))
```

```python
import functools
import math

import jax
import jax.numpy as jnp
import numpy as np
from jax import lax
from jax.experimental import pallas as pl
from jax.experimental.pallas import tpu as pltpu
from jax.sharding import PartitionSpec as P

NF = 30
ND = 64
NLON = 256
MAXSTEPS = 6
SRC_STEPS = 4
STEP_SIZE = 0.1
MESH = pl.DeviceIdType.MESH
HALF = ND // 2
TILES = 4
SLOTS = 8
F32 = jnp.float32
BF16 = jnp.bfloat16


def kernel(
    nlat, ncomp, group, spec_ref, mask_ref, nb_ref, steps_ref, cour_ref, cos_ref, sin_ref, op_ref,
    out_ref, w_ref, own_ref, halo_ref, code_ref, prop_ref, away_ref, got_ref, start_ref, state_ref,
    low_ref, inc_ref, home_ref,
    h_send, h_recv, w_send, w_recv, w_local, a_send, a_recv, b_send, b_recv,
):
    lat = lax.axis_index("lat")
    sub = lax.axis_index("sub")
    me = lax.axis_index("comp")
    bins, points = spec_ref.shape
    chunks, size = prop_ref.shape[0], prop_ref.shape[1]
    planes = size // 8
    share = points // ncomp
    total = bins * ncomp
    half_rows = total // 2
    first = me * bins
    last_lat = nlat - 1
    partner = {"sub": 1 - sub}

    barrier = pltpu.get_barrier_semaphore()
    peers = [partner]
    if nlat == 2:
        peers.append({"lat": 1 - lat})
    else:
        for move in (1, -1):
            peers.append({"lat": lax.rem(lat + move + nlat, nlat)})
            peers.append({"lat": lax.rem(lat + 2 * move + nlat, nlat), "sub": 1 - sub})
    for j in range(1, ncomp):
        peers.append({"comp": lax.rem(me + j, ncomp)})
    for peer in peers:
        pl.semaphore_signal(barrier, inc=1, device_id=peer, device_id_type=MESH)

    own_half = pl.ds(pl.multiple_of(sub * half_rows, 16), half_rows)
    load_w = pltpu.make_async_copy(op_ref, w_ref.at[own_half], w_local)
    load_w.start()

    lane = lax.broadcasted_iota(jnp.int32, (1, points), 1)
    column = lane & (NLON - 1)
    position = (lat * 2 + sub) * points + lane
    sea = mask_ref[...].astype(F32)
    west = (column - nb_ref[0:1, :]) & (NLON - 1)
    east = (nb_ref[1:2, :] - column) & (NLON - 1)

    def vertical(index_row):
        moved = ((index_row - column + 1) & (NLON - 1)) - 1
        return jnp.where(index_row == position, 2, moved)

    rows = lax.broadcasted_iota(jnp.int32, (size, points), 0)
    codes = jnp.zeros((size, points), F32)
    entries = [west, east, vertical(nb_ref[2:3, :]), vertical(nb_ref[3:4, :])]
    for k, entry in enumerate([e.astype(F32) for e in entries] + [sea]):
        codes = jnp.where(rows == k, jnp.broadcast_to(entry, (size, points)), codes)
    own_ref[0] = codes.astype(BF16)
    own_ref[1] = codes.astype(BF16)

    pl.semaphore_wait(barrier, len(peers))

    def kind(q):
        return lax.rem(lax.div(first + (q - 2) * size, HALF), 2)

    def has_from(ty, far):
        return jnp.where(ty == 0, lat >= far, lat <= last_lat - far)

    def has_to(ty, far):
        return jnp.where(ty == 0, lat <= last_lat - far, lat >= far)

    def pair_copy(q):
        return pltpu.make_async_remote_copy(
            src_ref=own_ref.at[q], dst_ref=halo_ref.at[0, q], send_sem=h_send.at[0, q],
            recv_sem=h_recv.at[0, q], device_id=partner, device_id_type=MESH)

    def side_copy(q, ty):
        to = jnp.clip(lat + 1 - 2 * ty, 0, last_lat)
        return pltpu.make_async_remote_copy(
            src_ref=own_ref.at[q], dst_ref=halo_ref.at[1, q], send_sem=h_send.at[1, q],
            recv_sem=h_recv.at[1, q], device_id={"lat": to}, device_id_type=MESH)

    def hand_copy(q, ty):
        slot = jnp.where(sub == ty, 2, 0)
        return pltpu.make_async_remote_copy(
            src_ref=halo_ref.at[1, q], dst_ref=halo_ref.at[slot, q], send_sem=h_send.at[2, q],
            recv_sem=h_recv.at[2, q], device_id=partner, device_id_type=MESH)

    def far_copy(q, ty):
        to = jnp.clip(lat + 2 - 4 * ty, 0, last_lat)
        return pltpu.make_async_remote_copy(
            src_ref=own_ref.at[q], dst_ref=halo_ref.at[2, q], send_sem=h_send.at[3, q],
            recv_sem=h_recv.at[3, q], device_id={"lat": to, "sub": 1 - sub}, device_id_type=MESH)

    def send_own(q, ty):
        @pl.when(has_to(ty, 1))
        def _():
            side_copy(q, ty).start()

        @pl.when(sub == ty)
        def _():
            pair_copy(q).start()

        if nlat > 2:
            @pl.when((sub != ty) & has_to(ty, 2))
            def _():
                far_copy(q, ty).start()

    def hand_on(q, ty):
        @pl.when(has_from(ty, 1))
        def _():
            side_copy(q, ty).wait_recv()
            hand_copy(q, ty).start()

    def arrive(q, ty):
        @pl.when(has_from(ty, 1))
        def _():
            hand_copy(q, ty).wait_recv()

        @pl.when(sub != ty)
        def _():
            pair_copy(q).wait_recv()

        if nlat > 2:
            @pl.when((sub == ty) & has_from(ty, 2))
            def _():
                far_copy(q, ty).wait_recv()

    def sent(q, ty):
        @pl.when(has_to(ty, 1))
        def _():
            side_copy(q, ty).wait_send()

        @pl.when(sub == ty)
        def _():
            pair_copy(q).wait_send()

        if nlat > 2:
            @pl.when((sub != ty) & has_to(ty, 2))
            def _():
                far_copy(q, ty).wait_send()

        @pl.when(has_from(ty, 1))
        def _():
            hand_copy(q, ty).wait_send()

    send_own(0, 0)
    send_own(1, 1)

    def prepare(i, carry):
        chunk = sea * spec_ref[pl.ds(pl.multiple_of(i * size, size), size), :]
        own_ref[i + 2] = chunk.astype(BF16)
        send_own(i + 2, kind(i + 2))
        return carry

    lax.fori_loop(0, chunks, prepare, 0)

    give_w = pltpu.make_async_remote_copy(
        src_ref=op_ref, dst_ref=w_ref.at[own_half], send_sem=w_send, recv_sem=w_recv,
        device_id=partner, device_id_type=MESH)
    give_w.start()

    for q in (0, 1):
        hand_on(q, q)
    ahead = min(6, chunks)
    for q in range(2, 2 + ahead):
        hand_on(q, kind(q))

    for ty in (0, 1):
        arrive(ty, ty)
        for slot in range(SLOTS):
            row = slot % 2 if ty == 0 else 1 - slot % 2
            cols = slice(row * NLON, (row + 1) * NLON)
            if slot < 6:
                part = halo_ref[2 - slot // 2, ty, :, cols].astype(F32)
            else:
                part = own_ref[ty, :, cols].astype(F32)
            for k, source in enumerate((0, 1, 2 + ty, 4)):
                code_ref[ty, slot, k] = jnp.broadcast_to(part[source:source + 1, :], (8, NLON))

    def propagate(i):
        q = i + 2
        ty = kind(q)

        @pl.when(i + ahead < chunks)
        def _():
            hand_on(q + ahead, kind(q + ahead))

        arrive(q, ty)
        bin0 = first + i * size
        freq = lax.div(bin0, ND)
        direction = lax.rem(bin0, ND)
        to_east = jnp.where((direction < ND // 4) | (direction >= 3 * ND // 4), 1, 0)
        steps = steps_ref[freq]
        speed = cour_ref[freq]
        sign = jnp.where(to_east == 1, 1.0, -1.0)
        shift1 = jnp.where(to_east == 1, 1, NLON - 1)
        shift2 = jnp.where(to_east == 1, 2, NLON - 2)
        back1 = NLON - shift1
        d8 = lax.div(direction, 8)
        abs_cos = cos_ref[pl.ds(d8, planes)]
        abs_sin = sin_ref[pl.ds(d8, planes)]

        def lanes(slot):
            row = jnp.where(ty == 0, slot % 2, 1 - slot % 2)
            return pl.ds(pl.multiple_of(row * NLON, NLON), NLON)

        values = []
        for slot in range(SLOTS):
            if slot < 6:
                part = halo_ref[2 - slot // 2, q, :, lanes(slot)].astype(F32)
            else:
                part = spec_ref[pl.ds(pl.multiple_of(i * size, size), size), lanes(slot)]
            part = part.reshape(planes, 8, NLON)
            if slot >= 6:
                part = part * code_ref[ty, slot, 3][None]
            values.append(part)
        for t in range(MAXSTEPS):
            live = jnp.where(t < steps, speed, 0.0)
            wx = live * abs_cos
            wy = live * abs_sin
            keep = 1.0 - wx - wy
            fresh = list(values)
            for slot in range(t + 1, SLOTS):
                x = values[slot]
                below = values[slot - 1]
                near = code_ref[ty, slot, 1 - to_east][None] == 1.0
                vert = code_ref[ty, slot, 2][None] * sign
                lon = jnp.where(near, pltpu.roll(x, shift1, 2), pltpu.roll(x, shift2, 2))
                up = jnp.where(vert == -1.0, pltpu.roll(below, shift1, 2),
                               jnp.where(vert == 1.0, pltpu.roll(below, back1, 2), below))
                up = jnp.where(jnp.abs(vert) == 2.0, x, up)
                fresh[slot] = code_ref[ty, slot, 3][None] * (keep * x + wx * lon + wy * up)
            values = fresh
        for slot in (6, 7):
            prop_ref[i, :, lanes(slot)] = values[slot].reshape(size, NLON)
        whole = prop_ref[i]
        for c in range(ncomp):
            away_ref[c, i] = whole[:, c * share:(c + 1) * share].astype(BF16)

    groups = chunks // group

    def out_copy(j, g):
        to = lax.rem(me + j, ncomp)
        span = pl.ds(g * group, group)
        return pltpu.make_async_remote_copy(
            src_ref=away_ref.at[to, span], dst_ref=got_ref.at[me, span],
            send_sem=a_send.at[j], recv_sem=a_recv.at[j],
            device_id={"comp": to}, device_id_type=MESH)

    def whole_copy(j):
        to = lax.rem(me + j, ncomp)
        return pltpu.make_async_remote_copy(
            src_ref=away_ref.at[to], dst_ref=got_ref.at[me],
            send_sem=a_send.at[j], recv_sem=a_recv.at[j],
            device_id={"comp": to}, device_id_type=MESH)

    def run_group(g, carry):
        def one(i, inner):
            propagate(g * group + i)
            return inner

        lax.fori_loop(0, group, one, 0)
        for j in range(1, ncomp):
            out_copy(j, g).start()
        return carry

    lax.fori_loop(0, groups, run_group, 0)

    for q in (0, 1):
        sent(q, q)

    def drain(q, carry):
        sent(q, kind(q))
        return carry

    lax.fori_loop(2, chunks + 2, drain, 0)
    got_ref[me] = away_ref[me]
    load_w.wait()
    give_w.wait()

    for j in range(1, ncomp):
        whole_copy(j).wait()
    for c in range(ncomp):
        start_ref[c * bins:(c + 1) * bins, :] = got_ref[c].astype(F32).reshape(bins, share)
    tile = total // TILES
    per_tile = bins // tile if bins >= tile else tile // bins
    for m in range(TILES):
        span = slice(m * tile, (m + 1) * tile)
        low_ref[0, span, :] = start_ref[span, :].astype(BF16)

    def tile_rows(m):
        return pl.ds(pl.multiple_of(m * tile, 16), tile)

    def advance(step, m):
        span = tile_rows(m)
        driving = jnp.dot(w_ref[span, :], low_ref[step % 2], preferred_element_type=F32)
        now = start_ref[span, :] if step == 0 else state_ref[span, :]
        return span, now + STEP_SIZE * now * driving

    for step in range(SRC_STEPS - 1):
        def one_tile(m, carry, step=step):
            span, now = advance(step, m)
            state_ref[span, :] = now
            low_ref[(step + 1) % 2, span, :] = now.astype(BF16)
            return carry

        lax.fori_loop(0, TILES, one_tile, 0)

    def home_copy(j, to):
        return pltpu.make_async_remote_copy(
            src_ref=inc_ref.at[to], dst_ref=home_ref.at[me],
            send_sem=b_send.at[j], recv_sem=b_recv.at[j],
            device_id={"comp": to}, device_id_type=MESH)

    mine = lax.div(me * TILES, ncomp)

    def last_tile(i, carry):
        m = lax.rem(mine + 1 + i, TILES)
        span, now = advance(SRC_STEPS - 1, m)
        gain = now - start_ref[span, :]
        for k in range(per_tile):
            to = m * per_tile + k
            inc_ref[to] = gain[k * bins:(k + 1) * bins, :].astype(BF16)
            j = lax.rem(to - me + ncomp, ncomp)

            @pl.when(to != me)
            def _():
                home_copy(j, to).start()

        return carry

    lax.fori_loop(0, TILES, last_tile, 0)
    home_ref[me] = inc_ref[me]
    for c in range(ncomp):
        j = lax.rem(me - c + ncomp, ncomp)

        @pl.when(me != c)
        def _():
            home_copy(j, lax.rem(me + j, ncomp)).wait()

        cols = slice(c * share, (c + 1) * share)
        before = prop_ref[:, :, cols].reshape(bins, share)
        out_ref[:, cols] = sea[:, cols] * (before + home_ref[c].astype(F32))


def solution(mesh):
    nlat, ncomp = mesh.shape["lat"], mesh.shape["comp"]

    def per_device(spectrum, sea_mask, neighbours, substeps, courant, source_operator):
        bins, points = spectrum.shape
        size = 16 if bins % 16 == 0 else 8
        chunks = bins // size
        group = 5 if chunks % 5 == 0 else 1
        share = points // ncomp
        total = bins * ncomp
        angles = (np.arange(ND, dtype=np.float32) + np.float32(0.5)) * np.float32(2.0 * math.pi / ND)
        spread = lambda v: jnp.asarray(
            np.broadcast_to(np.abs(v).astype(np.float32)[:, None], (ND, NLON)).reshape(ND // 8, 8, NLON))
        vmem = pl.BlockSpec(memory_space=pltpu.VMEM)
        smem = pl.BlockSpec(memory_space=pltpu.SMEM)
        kinds = 3 if nlat == 2 else 4
        return pl.pallas_call(
            functools.partial(kernel, nlat, ncomp, group),
            out_shape=jax.ShapeDtypeStruct((bins, points), F32),
            in_specs=[vmem, vmem, vmem, smem, smem, vmem, vmem, pl.BlockSpec(memory_space=pl.ANY)],
            out_specs=vmem,
            scratch_shapes=[
                pltpu.VMEM((total, total), BF16),
                pltpu.VMEM((chunks + 2, size, points), BF16),
                pltpu.VMEM((3, chunks + 2, size, points), BF16),
                pltpu.VMEM((2, SLOTS, 4, 8, NLON), F32),
                pltpu.VMEM((chunks, size, points), F32),
                pltpu.VMEM((ncomp, chunks, size, share), BF16),
                pltpu.VMEM((ncomp, chunks, size, share), BF16),
                pltpu.VMEM((total, share), F32),
                pltpu.VMEM((total, share), F32),
                pltpu.VMEM((2, total, share), BF16),
                pltpu.VMEM((ncomp, bins, share), BF16),
                pltpu.VMEM((ncomp, bins, share), BF16),
                pltpu.SemaphoreType.DMA((kinds, chunks + 2)),
                pltpu.SemaphoreType.DMA((kinds, chunks + 2)),
                pltpu.SemaphoreType.DMA,
                pltpu.SemaphoreType.DMA,
                pltpu.SemaphoreType.DMA,
                pltpu.SemaphoreType.DMA((ncomp,)),
                pltpu.SemaphoreType.DMA((ncomp,)),
                pltpu.SemaphoreType.DMA((ncomp,)),
                pltpu.SemaphoreType.DMA((ncomp,)),
            ],
            compiler_params=pltpu.CompilerParams(
                collective_id=0, has_side_effects=True, vmem_limit_bytes=56 * 1024 * 1024),
        )(spectrum, sea_mask.reshape(1, points), neighbours, substeps, courant,
          spread(np.cos(angles)), spread(np.sin(angles)), source_operator)

    placed = (
        P("comp", ("members", "lat", "sub")),
        P(("members", "lat", "sub")),
        P(None, ("members", "lat", "sub")),
        P(),
        P(),
        P("sub", None),
    )
    return jax.shard_map(
        per_device,
        mesh=mesh,
        in_specs=placed,
        out_specs=P("comp", ("members", "lat", "sub")),
        check_vma=False,
    )
```
